256 devices in a mesh: groups: 4 (over y, x), neuron: 64 (over z, core).
Axes of the slice: x: 2, y: 2, z: 32, core: 2. Of those that a mesh axis runs over, the one named last changes fastest.
The devices are a block of a 4x8x32 slice.
Arguments:
- queries: bfloat16 [2048, 8, 128], P(('groups', 'neuron')), parts along dimension 0, may hold values from -18 to 18
- keys: bfloat16 [2048, 1024, 128], P(('groups', 'neuron')), parts along dimension 0, may hold values from -6 to 6
- values: bfloat16 [2048, 1024, 128], P(('groups', 'neuron')), parts along dimension 0, may hold values from -6 to 6
- lengths: int32 [512], P('groups'), parts along dimension 0, may hold values from 256 to 1024
- active_blocks: int32 [64, 32], P('groups'), parts along dimension 0, may hold values from 0 to 111, all different within a row
- residual: bfloat16 [512, 4096], P('groups', 'neuron'), parts along dimension 0, may hold values from -18 to 18
- out_weight: bfloat16 [4096, 4096], P(None, 'neuron'), may hold values from -0.09375 to 0.09375
- norm_gain: bfloat16 [4096], P('neuron'), may hold values from 0.099609375 to 1.8984375
- gate_weight: bfloat16 [4096, 14336], P('neuron'), may hold values from -0.09375 to 0.09375
- up_weight: bfloat16 [4096, 14336], P('neuron'), may hold values from -0.09375 to 0.09375
- down_weight: bfloat16 [14336, 4096], P(None, 'neuron'), may hold values from -0.09375 to 0.09375
Outputs:
- layer_out: bfloat16 [512, 4096], P('groups', 'neuron'), parts along dimension 0
The draws below stay inside these ranges and needn't reach their ends.
There are 4 independent parts, one for each index of `groups`. The reference program is written for one: setup_inputs(seed, part) draws one part's arguments, and reference() takes and returns one part's arrays. A program takes and returns all parts, laid end to end along the dimension named above; an argument that names none is the same for every part. Nothing has to cross between parts.
Inputs may be any that keep to these rules, and one draw needn't show every extreme that they name: `active_blocks`: each row names 32 different blocks; every block is named by some row.
All inputs are finite; a program needn't handle non-finite values.
Results may differ from the reference program's by a relative error of at most 0.0052.
Values may be sent and summed in bfloat16 or wider, within the bound.
No kernel may reach another device: no remote copies, remote signals or barrier semaphores. Data moves between devices by JAX's collectives and lax.ppermute only.
A program may use at most 64 MiB of HBM per device.

```python
import jax
import jax.numpy as jnp
from jax import lax

D = 4096
KVH = 4
GQ = 8
HD = 128
BLK = 128
NBLK = 112
ACT = 32
G = 16
ROWS = 128
LEN = 1024
H = 32
FF = 14336


def draw_keys(key, part):
    normal = jnp.clip(jax.random.normal(jax.random.fold_in(key, 11), (KVH * ROWS, LEN, HD), jnp.float32), -6.0, 6.0)
    return normal.astype(jnp.bfloat16)


def draw_queries(key, part):
    picked = jnp.clip(3.0 * jax.random.normal(jax.random.fold_in(key, 13), (KVH * ROWS, GQ, HD), jnp.float32), -18.0, 18.0)
    return picked.astype(jnp.bfloat16)


def draw_residual(key, part):
    columns = jnp.arange(D, dtype=jnp.float32) / D
    rough = jax.random.uniform(jax.random.fold_in(key, 17), (D,), jnp.float32, 0.6, 1.4)
    column_scale = 0.5 * jnp.exp(jnp.log(3.0) * columns) * rough
    base = jnp.clip(jax.random.normal(jax.random.fold_in(key, 19), (ROWS, D), jnp.float32), -4.0, 4.0)
    return jnp.clip(base * column_scale[None, :], -18.0, 18.0).astype(jnp.bfloat16)


def set_ends(entries, stream_key, smallest, top_value):
    extent = entries.shape
    spot = [jax.random.randint(jax.random.fold_in(stream_key, axis), (), 0, extent[axis]) for axis in range(len(extent))]
    entries = entries.at[tuple(spot)].set(smallest)
    longest = extent.index(max(extent))
    spot[longest] = (spot[longest] + 1) % extent[longest]
    return entries.at[tuple(spot)].set(top_value)


def steps_of(key, shape, pieces, low, high):
    level = 1.0
    for position, parts in pieces:
        steps = jax.random.uniform(jax.random.fold_in(jax.random.fold_in(key, 6), position), (parts,), jnp.float32, low / len(pieces), high / len(pieces))
        level = level * jnp.repeat(jnp.exp(steps), shape[position] // parts).reshape((-1,) + (1,) * (len(shape) - 1 - position))
    return level


def different_ones(rng, rows, amount, top, lift):
    ranking = jax.random.permutation(jax.random.fold_in(rng, 1), amount)
    boost = ranking
    for power in range(3):
        boost = boost * boost // amount
    boost = boost * lift // amount
    lots = jax.random.randint(jax.random.fold_in(rng, 2), (rows, amount), 0, 4096) + boost
    fixed_rows = jax.random.permutation(jax.random.fold_in(rng, 3), rows)[jnp.arange(amount) % rows]
    lots = jnp.where(jnp.arange(rows)[:, None] == fixed_rows[None, :], 1 << 14, lots)
    score = lots * amount + jnp.arange(amount)
    return lax.top_k(score.astype(jnp.int32), top)[1].astype(jnp.int32)


def noise(own_key, dims, spread, reach, pieces=(), kind=jnp.bfloat16):
    entries = jax.random.normal(own_key, dims, jnp.float32) * spread
    if len(pieces) > 0:
        entries = steps_of(own_key, dims, pieces, -0.22, 0.18) * entries
    return jnp.clip(entries, min=-reach, max=reach).astype(kind)


def setup_inputs(seed: int = 0, part: int = 0) -> dict:
    key_list = jax.random.split(jax.random.key(seed), 12)
    own_keys = jax.random.split(jax.random.fold_in(key_list[11], part), 12)
    queries = draw_queries(jax.random.fold_in(jax.random.fold_in(key_list[11], part), 71), part)
    keys = draw_keys(jax.random.fold_in(jax.random.fold_in(key_list[11], part), 71), part)
    values = noise(own_keys[2], (KVH * ROWS, LEN, HD), 1.0, 6.0, ((0, 64),))
    lengths = set_ends(jax.random.randint(own_keys[3], (ROWS,), LEN // 4, LEN + 1), jax.random.fold_in(own_keys[3], 1), LEN // 4, LEN).astype(jnp.int32)
    active_blocks = different_ones(own_keys[4], G, NBLK, ACT, 2340)
    residual = draw_residual(jax.random.fold_in(jax.random.fold_in(key_list[11], part), 71), part)
    out_weight = noise(key_list[6], (H * HD, D), (H * HD) ** -0.5, 0.09375, ((1, 64),))
    norm_gain = jnp.clip(1.0 + 0.18 * jax.random.normal(key_list[7], (D,), jnp.float32), 0.099609375, 1.8984375).astype(jnp.bfloat16)
    gate_weight = noise(key_list[8], (D, FF), D ** -0.5, 0.09375, ((0, 64),))
    up_weight = noise(key_list[9], (D, FF), D ** -0.5, 0.09375, ((0, 64),))
    down_weight = noise(key_list[10], (FF, D), (ACT * BLK) ** -0.5, 0.09375, ((1, 64),))
    return {"queries": queries, "keys": keys, "values": values, "lengths": lengths, "active_blocks": active_blocks, "residual": residual, "out_weight": out_weight, "norm_gain": norm_gain, "gate_weight": gate_weight, "up_weight": up_weight, "down_weight": down_weight}


def reference(queries, keys, values, lengths, active_blocks, residual, out_weight, norm_gain, gate_weight, up_weight, down_weight):
    entry_rows = jnp.arange(KVH * ROWS, dtype=jnp.int32) % ROWS
    live_lengths = lengths[entry_rows]
    scores = jnp.einsum('egc,etc->egt', queries.astype(jnp.float32), keys.astype(jnp.float32)) * HD ** (-0.5)
    live_mask = jnp.arange(LEN, dtype=jnp.int32)[None, None, :] < live_lengths[:, None, None]
    scores = jnp.where(live_mask, scores, -1e+30)
    running_max = lax.optimization_barrier(jnp.max(scores, axis=-1, keepdims=True))
    weights = jnp.where(live_mask, jnp.exp(scores - running_max), 0.0)
    probs = (weights / lax.optimization_barrier(jnp.sum(weights, axis=-1, keepdims=True))).astype(jnp.bfloat16)
    attended = jnp.einsum('egt,etc->egc', probs.astype(jnp.float32), values.astype(jnp.float32)).astype(jnp.bfloat16)
    by_head = attended.reshape(KVH, ROWS, GQ * HD)
    out_heads = out_weight.reshape(KVH, GQ * HD, D)
    stream = residual.astype(jnp.float32) + jnp.einsum('hrc,hcd->rd', by_head.astype(jnp.float32), out_heads.astype(jnp.float32))
    square_sums = lax.optimization_barrier(jnp.sum(stream * stream, axis=1))
    normed = (stream * lax.rsqrt(square_sums / D + 1e-05)[:, None] * norm_gain.astype(jnp.float32)).astype(jnp.bfloat16)
    group_rows = ROWS // G

    def one_group(operand):
        rows_in, picked = operand
        columns = (picked[:, None] * BLK + jnp.arange(BLK, dtype=jnp.int32)[None, :]).reshape(-1).astype(jnp.int32)
        gate_part = jnp.dot(rows_in, jnp.take(gate_weight, columns, axis=1), preferred_element_type=jnp.float32)
        up_part = jnp.dot(rows_in, jnp.take(up_weight, columns, axis=1), preferred_element_type=jnp.float32)
        activated = (jnp.maximum(gate_part, 0.0) * up_part).astype(jnp.bfloat16)
        return jnp.dot(activated, jnp.take(down_weight, columns, axis=0), preferred_element_type=jnp.float32)
    down_part = lax.map(one_group, (normed.reshape(G, group_rows, D), active_blocks)).reshape(ROWS, D)
    return (stream + down_part).astype(jnp.bfloat16)
```

```python
import jax
import jax.numpy as jnp
import numpy as np
from jax import lax
from jax.experimental import pallas as pl
from jax.experimental.pallas import tpu as pltpu
from jax.sharding import Mesh
from jax.sharding import PartitionSpec as P

D = 4096
BLK = 128
ROWS = 128
FAR, NEAR = 8, 4
DEVICES = FAR * NEAR * 2
SHARE = 8
LANES = 128
CHUNKS = 7
VMEM_LIMIT = 55 * 1024 * 1024
AXES = ("far", "near", "core")
ALL = ("groups",) + AXES
f32, bf16 = jnp.float32, jnp.bfloat16

NEAR_STEPS = ((0, 0), (1, 1), (2, -2), (-1, -1))
MID_STEPS = ((0, 0), (NEAR, -NEAR))
FAR_STEPS = ((0, 0), (2 * NEAR, 2 * NEAR), (-2 * NEAR, -2 * NEAR), (4 * NEAR, -4 * NEAR))


def moved(n, steps, sign=1):
    z, c = divmod(n, 2)
    return (z + sign * steps[c]) % (FAR * NEAR) * 2 + c


def along_z(x, steps):
    return lax.ppermute(x, AXES, [(n, moved(n, steps)) for n in range(DEVICES)])


def other_core(x):
    return lax.ppermute(x, AXES, [(n, n ^ 1) for n in range(DEVICES)])


def gathered(x):
    mine = lax.all_gather(x, "far", axis=0)
    mine = jnp.stack([mine] + [along_z(mine, steps) for steps in NEAR_STEPS[1:]])
    return mine, other_core(mine)


def arrival(n):
    order = []
    for x in range(2):
        for steps in NEAR_STEPS:
            z, c = divmod(moved(n ^ x, steps, -1), 2)
            order += [(a * NEAR + z % NEAR) * 2 + c for a in range(FAR)]
    return order


def summed(kept, sent):
    kept = kept + other_core(sent).astype(f32)
    sent = kept.astype(bf16)
    got = [along_z(sent[s], NEAR_STEPS[s]) for s in (2, 1, 3)]
    kept = kept[0] + got[0].astype(f32) + got[1].astype(f32) + got[2].astype(f32)
    half = FAR // 2
    on, back = kept[half].astype(bf16), kept[half + 1].astype(bf16)
    for k in range(half - 1, 0, -1):
        on = (along_z(on, (NEAR, -NEAR)).astype(f32) + kept[k]).astype(bf16)
        if k > 1:
            back = (along_z(back, (-NEAR, NEAR)).astype(f32) + kept[FAR + 1 - k]).astype(bf16)
    return kept[0] + along_z(on, (NEAR, -NEAR)).astype(f32) + along_z(back, (-NEAR, NEAR)).astype(f32)


def departure(n):
    return [
        moved(moved(n ^ x, steps), (NEAR * k, -NEAR * k))
        for x in range(2)
        for steps in NEAR_STEPS
        for k in range(FAR)
    ]


def whole_attention(queries, keys, values, live_lengths, score_scale):
    scores = jnp.einsum("egc,etc->egt", queries, keys, preferred_element_type=f32) * score_scale
    live_mask = (
        jnp.arange(keys.shape[1], dtype=jnp.int32)[None, None, :] < live_lengths[:, None, None]
    )
    scores = jnp.where(live_mask, scores, -1e30)
    running_max = jnp.max(scores, axis=-1, keepdims=True)
    weights = jnp.where(live_mask, jnp.exp(scores - running_max), 0.0)
    probs = (weights / jnp.sum(weights, axis=-1, keepdims=True)).astype(bf16)
    return jnp.einsum("egt,etc->egc", probs, values, preferred_element_type=f32).astype(bf16)


def nt_dot(a, b):
    return lax.dot_general(a, b, (((1,), (1,)), ((), ())), preferred_element_type=f32)


def rows_of(g):
    return pl.ds(pl.multiple_of(g * SHARE, SHARE), SHARE)


def up_kernel(
    order, active, mine, theirs, residual, out_t, gain, gate, up,
    stream, kept, sent, heads, squares, gates, ups, both, arrived,
):
    groups = active.shape[0]
    half = DEVICES // 2
    cols = gate.shape[1] // CHUNKS
    copies = []
    for i in range(CHUNKS):
        at = pl.ds(i * cols, cols)
        copies.append([
            pltpu.make_async_copy(gate.at[:, at], gates.at[:, at], arrived.at[0, i]),
            pltpu.make_async_copy(up.at[:, at], ups.at[:, at], arrived.at[1, i]),
        ])
        for copy in copies[-1]:
            copy.start()

    for x, buf in enumerate((mine, theirs)):

        @pl.loop(0, half)
        def _(i):
            device = order[0, x * half + i]
            heads[device // groups, lax.rem(device, groups)] = buf[i].astype(f32)

    width = heads.shape[-1]
    total = residual[...].astype(f32)
    for h in range(heads.shape[0]):
        lhs = heads[h].reshape(ROWS, width).astype(bf16)
        total += nt_dot(lhs, out_t[:, h * width : (h + 1) * width])
    stream[...] = total
    lane = lax.broadcasted_iota(jnp.int32, (ROWS, LANES), 1).astype(f32)
    ones = 1.0 + lane / LANES
    squares[...] = jnp.sum(total * total, axis=1, keepdims=True) * ones
    scaled = total * gain[...]
    high = scaled.astype(bf16)
    low = (scaled - high.astype(f32)).astype(bf16)
    lhs = jnp.concatenate([high, low], axis=1)

    for i in range(CHUNKS):
        for t, w in enumerate((gates, ups)):
            copies[i][t].wait()
            rhs = w[:, i * cols : (i + 1) * cols]
            out = jnp.dot(lhs, jnp.concatenate([rhs, rhs], axis=0), preferred_element_type=f32)
            for j in range(cols // BLK):
                both[i * (cols // BLK) + j, :, t * BLK : (t + 1) * BLK] = out[:, j * BLK : (j + 1) * BLK]

    for x, to in enumerate((kept, sent)):

        @pl.loop(0, half)
        def _(i):
            device = order[1, x * half + i]
            q, g = device // groups, lax.rem(device, groups)
            rows = rows_of(g)
            for j in range(SHARE):
                tile = both[active[g, q * SHARE + j], rows, :].astype(to.dtype)
                to[i, :, j * BLK : (j + 1) * BLK] = tile[:, :BLK]
                to[i, :, (SHARE + j) * BLK : (SHARE + j + 1) * BLK] = tile[:, BLK:]
            to[i, :, 2 * SHARE * BLK :] = squares[rows, :].astype(to.dtype)


def down_kernel(order, active, mine, theirs, stream_t, down_hbm, out_t, dense, down_t, arrived):
    groups = active.shape[0]
    half = DEVICES // 2
    cols = down_t.shape[1] // CHUNKS
    copies = []
    for i in range(CHUNKS):
        at = pl.ds(i * cols, cols)
        copies.append(pltpu.make_async_copy(down_hbm.at[:, at], down_t.at[:, at], arrived.at[i]))
        copies[-1].start()
    dense[...] = jnp.zeros_like(dense)
    for x, buf in enumerate((mine, theirs)):

        @pl.loop(0, half)
        def _(i):
            device = order[0, x * half + i]
            q, g = device // groups, lax.rem(device, groups)
            rows = rows_of(g)
            tile = buf[i].astype(f32)
            for j in range(SHARE):
                dense[active[g, q * SHARE + j], rows, :] = tile[:, j * BLK : (j + 1) * BLK]

    total = stream_t[...]
    per = 4
    for k in range(dense.shape[0] // per):
        if k * per * BLK % cols == 0:
            copies[k * per * BLK // cols].wait()
        rhs = jnp.concatenate([dense[k * per + j].astype(bf16) for j in range(per)], axis=1)
        total += nt_dot(down_t[:, k * per * BLK : (k + 1) * per * BLK], rhs)
    out_t[...] = total.astype(out_t.dtype)


SMEM = pl.BlockSpec(memory_space=pltpu.SMEM)
VMEM = pl.BlockSpec(memory_space=pltpu.VMEM)
HBM = pl.BlockSpec(memory_space=pltpu.HBM)


def body(
    queries,
    keys,
    values,
    lengths,
    active_blocks,
    residual,
    out_weight,
    norm_gain,
    gate_weight,
    up_weight,
    down_weight,
):
    entries = keys.shape[0]
    me = lax.axis_index(AXES)
    tables = np.array([[arrival(n), departure(n)] for n in range(DEVICES)], np.int32)
    order = lax.dynamic_index_in_dim(jnp.asarray(tables), me, keepdims=False)
    live_lengths = lax.dynamic_slice_in_dim(lengths, (me * entries) % ROWS, entries)
    attended = whole_attention(queries, keys, values, live_lengths, queries.shape[2] ** (-0.5))
    mine, theirs = gathered(attended.reshape(entries, -1))

    width = residual.shape[1]
    half = DEVICES // 2
    features = mine.shape[-1]
    share_cols = 2 * SHARE * BLK + LANES
    flat = (half, SHARE, features)
    stream, kept, sent = pl.pallas_call(
        up_kernel,
        in_specs=[SMEM, SMEM, VMEM, VMEM, VMEM, VMEM, VMEM, HBM, HBM],
        out_specs=[VMEM, VMEM, VMEM],
        out_shape=[
            jax.ShapeDtypeStruct((ROWS, width), f32),
            jax.ShapeDtypeStruct((half, SHARE, share_cols), f32),
            jax.ShapeDtypeStruct((half, SHARE, share_cols), bf16),
        ],
        scratch_shapes=[
            pltpu.VMEM((out_weight.shape[0] // features, ROWS // SHARE, SHARE, features), f32),
            pltpu.VMEM((ROWS, LANES), f32),
            pltpu.VMEM(gate_weight.shape, bf16),
            pltpu.VMEM(up_weight.shape, bf16),
            pltpu.VMEM((gate_weight.shape[1] // BLK, ROWS, 2 * BLK), f32),
            pltpu.SemaphoreType.DMA((2, CHUNKS)),
        ],
        compiler_params=pltpu.CompilerParams(vmem_limit_bytes=VMEM_LIMIT),
        name="up_kernel",
    )(
        order,
        active_blocks,
        mine.reshape(flat),
        theirs.reshape(flat),
        residual,
        out_weight.T,
        norm_gain.astype(f32).reshape(1, width),
        gate_weight,
        up_weight,
    )

    terms = (NEAR, FAR, SHARE, share_cols)
    share = summed(kept.reshape(terms), sent.reshape(terms))
    cols = SHARE * BLK
    weights = 1.0 + jnp.arange(LANES, dtype=f32) / LANES
    square_sums = jnp.sum(share[:, 2 * cols :], axis=1, keepdims=True) / jnp.sum(weights)
    inverse = 1.0 / (square_sums / D + 1e-05)
    activated = jnp.maximum(share[:, :cols], 0.0) * share[:, cols : 2 * cols] * inverse
    mine, theirs = gathered(activated.astype(bf16))

    return pl.pallas_call(
        down_kernel,
        in_specs=[SMEM, SMEM, VMEM, VMEM, VMEM, HBM],
        out_specs=VMEM,
        out_shape=jax.ShapeDtypeStruct((width, ROWS), bf16),
        scratch_shapes=[
            pltpu.VMEM((down_weight.shape[0] // BLK, ROWS, BLK), f32),
            pltpu.VMEM((width, down_weight.shape[0]), bf16),
            pltpu.SemaphoreType.DMA((CHUNKS,)),
        ],
        compiler_params=pltpu.CompilerParams(vmem_limit_bytes=VMEM_LIMIT),
        name="down_kernel",
    )(order, active_blocks, mine.reshape(flat), theirs.reshape(flat), stream.T, down_weight.T).T


def solution(mesh):
    split = Mesh(mesh.devices.reshape(mesh.shape["groups"], FAR, NEAR, 2), ALL)
    return jax.shard_map(
        body,
        mesh=split,
        in_specs=(
            P(ALL, None, None),
            P(ALL, None, None),
            P(ALL, None, None),
            P("groups"),
            P("groups", None),
            P("groups", AXES),
            P(None, AXES),
            P(AXES),
            P(AXES, None),
            P(AXES, None),
            P(None, AXES),
        ),
        out_specs=P("groups", AXES),
        check_vma=False,
    )
```

```python
import jax
import jax.numpy as jnp
import numpy as np
from jax import lax
from jax.experimental import pallas as pl
from jax.experimental.pallas import tpu as pltpu
from jax.sharding import Mesh
from jax.sharding import PartitionSpec as P

D = 4096
BLK = 128
ROWS = 128
FAR, NEAR = 8, 4
DEVICES = FAR * NEAR * 2
SHARE = 8
LANES = 128
CHUNKS = 7
VMEM_LIMIT = 55 * 1024 * 1024
AXES = ("far", "near", "core")
ALL = ("groups",) + AXES
f32, bf16 = jnp.float32, jnp.bfloat16

SENSE = (-1, 1)
STEPS = ((0, 1, 2, 3), (4, 1, 2, 3))
TWO_AWAY = ((1, slice(2, 4)), (-1, slice(1, 3)))


def along_z(x, steps, cores=(0, 1)):
    chips = FAR * NEAR
    pairs = [(2 * z + c, (z + steps[c]) % chips * 2 + c) for z in range(chips) for c in cores]
    return lax.ppermute(x, AXES, pairs)


def passed_on(x, cores=(0, 1)):
    return along_z(x, (-NEAR, NEAR), cores)


def two_away(x):
    return [along_z(x[part], (-2 * way, 2 * way)) for way, part in TWO_AWAY]


def other_core(x):
    return lax.ppermute(x, "core", [(0, 1), (1, 0)])


def of_core(first, second):
    return jnp.where(lax.axis_index("core") == 0, first, second)


def gathered(pair):
    held = [pair]
    for k in range(3):
        held.append(passed_on(held[-1]))
    held[0] = of_core(pair, passed_on(held[-1], (1,)))
    far = jnp.stack(held)
    near = [far, along_z(far, (1, 1)), jnp.concatenate(two_away(far)), along_z(far, (-1, -1))]
    near = jnp.stack(near)
    return near, other_core(near)


def places(z, core, sign):
    sense, steps = SENSE[core], STEPS[core]
    near = [(0, steps), (sign, steps)]
    near += [(2 * sign * way * sense, steps[part]) for way, part in TWO_AWAY] + [(-sign, steps)]
    return [(z + d + sign * sense * NEAR * k) % (FAR * NEAR) for d, ks in near for k in ks]


def devices(n, sign):
    cores = [n % 2, 1 - n % 2]
    return [z * 2 + (c ^ p) for c in cores for z in places(n // 2, c, sign) for p in range(2)]


def arrival(n):
    return devices(n, -1)


def departure(n):
    return devices(n, 1)


def summed(kept, sent):
    kept = kept + other_core(sent).astype(f32)
    sent = kept.astype(bf16)
    with_it, against = two_away_terms(sent[2])
    up, down = along_z(sent[1], (1, 1)), along_z(sent[3], (-1, -1))
    terms = [kept[0, k] + up[k].astype(f32) + down[k].astype(f32) for k in range(4)]
    terms[1] += against[0].astype(f32)
    terms[2] += with_it[0].astype(f32) + against[1].astype(f32)
    terms[3] += with_it[1].astype(f32)
    total = passed_on(terms[0].astype(bf16), (1,)).astype(f32)
    for k in (3, 2, 1):
        total = passed_on((total + terms[k]).astype(bf16)).astype(f32)
    total += of_core(terms[0], 0.0)
    return total + other_core(total)[::-1]


def two_away_terms(x):
    return [along_z(x[2 * i : 2 * i + 2], (-2 * way, 2 * way)) for i, (way, _) in enumerate(TWO_AWAY)]


def whole_attention(queries, keys, values, live_lengths, score_scale):
    scores = jnp.einsum("egc,etc->egt", queries, keys, preferred_element_type=f32) * score_scale
    live_mask = (
        jnp.arange(keys.shape[1], dtype=jnp.int32)[None, None, :] < live_lengths[:, None, None]
    )
    scores = jnp.where(live_mask, scores, -1e30)
    running_max = jnp.max(scores, axis=-1, keepdims=True)
    weights = jnp.where(live_mask, jnp.exp(scores - running_max), 0.0)
    probs = (weights / jnp.sum(weights, axis=-1, keepdims=True)).astype(bf16)
    return jnp.einsum("egt,etc->egc", probs, values, preferred_element_type=f32).astype(bf16)


def nt_dot(a, b):
    return lax.dot_general(a, b, (((1,), (1,)), ((), ())), preferred_element_type=f32)


def rows_of(g):
    return pl.ds(pl.multiple_of(g * SHARE, SHARE), SHARE)


def up_kernel(
    order, active, mine, theirs, residual, out_t, gain, gate, up,
    stream, kept, sent, heads, squares, gates, ups, both, arrived,
):
    groups = active.shape[0]
    half = DEVICES // 2
    cols = gate.shape[1] // CHUNKS
    copies = []
    for i in range(CHUNKS):
        at = pl.ds(i * cols, cols)
        copies.append([
            pltpu.make_async_copy(gate.at[:, at], gates.at[:, at], arrived.at[0, i]),
            pltpu.make_async_copy(up.at[:, at], ups.at[:, at], arrived.at[1, i]),
        ])
        for copy in copies[-1]:
            copy.start()

    for x, buf in enumerate((mine, theirs)):

        @pl.loop(0, half)
        def _(i):
            device = order[0, x * half + i]
            heads[device // groups, lax.rem(device, groups)] = buf[i].astype(f32)

    width = heads.shape[-1]
    total = residual[...].astype(f32)
    for h in range(heads.shape[0]):
        lhs = heads[h].reshape(ROWS, width).astype(bf16)
        total += nt_dot(lhs, out_t[:, h * width : (h + 1) * width])
    stream[...] = total
    lane = lax.broadcasted_iota(jnp.int32, (ROWS, LANES), 1).astype(f32)
    ones = 1.0 + lane / LANES
    squares[...] = jnp.sum(total * total, axis=1, keepdims=True) * ones
    scaled = total * gain[...]
    high = scaled.astype(bf16)
    low = (scaled - high.astype(f32)).astype(bf16)
    lhs = jnp.concatenate([high, low], axis=1)

    for i in range(CHUNKS):
        for t, w in enumerate((gates, ups)):
            copies[i][t].wait()
            rhs = w[:, i * cols : (i + 1) * cols]
            out = jnp.dot(lhs, jnp.concatenate([rhs, rhs], axis=0), preferred_element_type=f32)
            for j in range(cols // BLK):
                both[i * (cols // BLK) + j, :, t * BLK : (t + 1) * BLK] = out[:, j * BLK : (j + 1) * BLK]

    for x, to in enumerate((kept, sent)):

        @pl.loop(0, half)
        def _(i):
            device = order[1, x * half + i]
            q, g = device // groups, lax.rem(device, groups)
            rows = rows_of(g)
            for j in range(SHARE):
                tile = both[active[g, q * SHARE + j], rows, :].astype(to.dtype)
                to[i, :, j * BLK : (j + 1) * BLK] = tile[:, :BLK]
                to[i, :, (SHARE + j) * BLK : (SHARE + j + 1) * BLK] = tile[:, BLK:]
            to[i, :, 2 * SHARE * BLK :] = squares[rows, :].astype(to.dtype)


def down_kernel(order, active, mine, theirs, stream_t, down_hbm, out_t, dense, down_t, arrived):
    groups = active.shape[0]
    half = DEVICES // 2
    cols = down_t.shape[1] // CHUNKS
    copies = []
    for i in range(CHUNKS):
        at = pl.ds(i * cols, cols)
        copies.append(pltpu.make_async_copy(down_hbm.at[:, at], down_t.at[:, at], arrived.at[i]))
        copies[-1].start()
    dense[...] = jnp.zeros_like(dense)
    for x, buf in enumerate((mine, theirs)):

        @pl.loop(0, half)
        def _(i):
            device = order[0, x * half + i]
            q, g = device // groups, lax.rem(device, groups)
            rows = rows_of(g)
            tile = buf[i].astype(f32)
            for j in range(SHARE):
                dense[active[g, q * SHARE + j], rows, :] = tile[:, j * BLK : (j + 1) * BLK]

    total = stream_t[...]
    per = 4
    for k in range(dense.shape[0] // per):
        if k * per * BLK % cols == 0:
            copies[k * per * BLK // cols].wait()
        rhs = jnp.concatenate([dense[k * per + j].astype(bf16) for j in range(per)], axis=1)
        total += nt_dot(down_t[:, k * per * BLK : (k + 1) * per * BLK], rhs)
    out_t[...] = total.astype(out_t.dtype)


SMEM = pl.BlockSpec(memory_space=pltpu.SMEM)
VMEM = pl.BlockSpec(memory_space=pltpu.VMEM)
HBM = pl.BlockSpec(memory_space=pltpu.HBM)


def body(
    queries,
    keys,
    values,
    lengths,
    active_blocks,
    residual,
    out_weight,
    norm_gain,
    gate_weight,
    up_weight,
    down_weight,
):
    entries = keys.shape[0]
    me = lax.axis_index(AXES)
    tables = np.array([[arrival(n), departure(n)] for n in range(DEVICES)], np.int32)
    order = lax.dynamic_index_in_dim(jnp.asarray(tables), me, keepdims=False)
    live_lengths = lax.dynamic_slice_in_dim(lengths, (me * entries) % ROWS, entries)
    attended = whole_attention(queries, keys, values, live_lengths, queries.shape[2] ** (-0.5))
    attended = attended.reshape(entries, -1)
    mine, theirs = gathered(jnp.stack([attended, other_core(attended)]))

    width = residual.shape[1]
    half = DEVICES // 2
    features = mine.shape[-1]
    share_cols = 2 * SHARE * BLK + LANES
    flat = (half, SHARE, features)
    stream, kept, sent = pl.pallas_call(
        up_kernel,
        in_specs=[SMEM, SMEM, VMEM, VMEM, VMEM, VMEM, VMEM, HBM, HBM],
        out_specs=[VMEM, VMEM, VMEM],
        out_shape=[
            jax.ShapeDtypeStruct((ROWS, width), f32),
            jax.ShapeDtypeStruct((half, SHARE, share_cols), f32),
            jax.ShapeDtypeStruct((half, SHARE, share_cols), bf16),
        ],
        scratch_shapes=[
            pltpu.VMEM((out_weight.shape[0] // features, ROWS // SHARE, SHARE, features), f32),
            pltpu.VMEM((ROWS, LANES), f32),
            pltpu.VMEM(gate_weight.shape, bf16),
            pltpu.VMEM(up_weight.shape, bf16),
            pltpu.VMEM((gate_weight.shape[1] // BLK, ROWS, 2 * BLK), f32),
            pltpu.SemaphoreType.DMA((2, CHUNKS)),
        ],
        compiler_params=pltpu.CompilerParams(vmem_limit_bytes=VMEM_LIMIT),
        name="up_kernel",
    )(
        order,
        active_blocks,
        mine.reshape(flat),
        theirs.reshape(flat),
        residual,
        out_weight.T,
        norm_gain.astype(f32).reshape(1, width),
        gate_weight,
        up_weight,
    )

    terms = (NEAR, FAR // 2, 2, SHARE, share_cols)
    share = summed(kept.reshape(terms), sent.reshape(terms))
    cols = SHARE * BLK
    weights = 1.0 + jnp.arange(LANES, dtype=f32) / LANES
    square_sums = jnp.sum(share[..., 2 * cols :], axis=-1, keepdims=True) / jnp.sum(weights)
    inverse = 1.0 / (square_sums / D + 1e-05)
    activated = jnp.maximum(share[..., :cols], 0.0) * share[..., cols : 2 * cols] * inverse
    mine, theirs = gathered(activated.astype(bf16))

    return pl.pallas_call(
        down_kernel,
        in_specs=[SMEM, SMEM, VMEM, VMEM, VMEM, HBM],
        out_specs=VMEM,
        out_shape=jax.ShapeDtypeStruct((width, ROWS), bf16),
        scratch_shapes=[
            pltpu.VMEM((down_weight.shape[0] // BLK, ROWS, BLK), f32),
            pltpu.VMEM((width, down_weight.shape[0]), bf16),
            pltpu.SemaphoreType.DMA((CHUNKS,)),
        ],
        compiler_params=pltpu.CompilerParams(vmem_limit_bytes=VMEM_LIMIT),
        name="down_kernel",
    )(order, active_blocks, mine.reshape(flat), theirs.reshape(flat), stream.T, down_weight.T).T


def solution(mesh):
    split = Mesh(mesh.devices.reshape(mesh.shape["groups"], FAR, NEAR, 2), ALL)
    return jax.shard_map(
        body,
        mesh=split,
        in_specs=(
            P(ALL, None, None),
            P(ALL, None, None),
            P(ALL, None, None),
            P("groups"),
            P("groups", None),
            P("groups", AXES),
            P(None, AXES),
            P(AXES),
            P(AXES, None),
            P(AXES, None),
            P(None, AXES),
        ),
        out_specs=P("groups", AXES),
        check_vma=False,
    )
```

```python
import jax
import jax.numpy as jnp
import numpy as np
from jax import lax
from jax.experimental import pallas as pl
from jax.experimental.pallas import tpu as pltpu
from jax.sharding import Mesh
from jax.sharding import PartitionSpec as P

D = 4096
BLK = 128
ROWS = 128
FAR, NEAR = 8, 4
DEVICES = FAR * NEAR * 2
SHARE = 8
LANES = 128
CHUNKS = 7
VMEM_LIMIT = 55 * 1024 * 1024
UNROLL = 4
AXES = ("far", "near", "core")
ALL = ("groups",) + AXES
f32, bf16 = jnp.float32, jnp.bfloat16

SENSE = (-1, 1)
STEPS = ((0, 1, 2, 3), (4, 1, 2, 3))
TWO_AWAY = ((1, slice(2, 4)), (-1, slice(1, 3)))


def along_z(x, steps, cores=(0, 1)):
    chips = FAR * NEAR
    pairs = [(2 * z + c, (z + steps[c]) % chips * 2 + c) for z in range(chips) for c in cores]
    return lax.ppermute(x, AXES, pairs)


def passed_on(x, cores=(0, 1)):
    return along_z(x, (-NEAR, NEAR), cores)


def two_away(x):
    return [along_z(x[part], (-2 * way, 2 * way)) for way, part in TWO_AWAY]


def other_core(x):
    return lax.ppermute(x, "core", [(0, 1), (1, 0)])


def of_core(first, second):
    return jnp.where(lax.axis_index("core") == 0, first, second)


def gathered(pair, ready=None):
    held = [pair, passed_on(pair)]
    if ready is not None:
        held[1], ready = lax.optimization_barrier((held[1], ready))
    for k in range(2):
        held.append(passed_on(held[-1]))
    held[0] = of_core(pair, passed_on(held[-1], (1,)))
    far = jnp.stack(held)
    near = [far, along_z(far, (1, 1)), jnp.concatenate(two_away(far)), along_z(far, (-1, -1))]
    near = jnp.stack(near)
    return near, other_core(near), ready


def places(z, core, sign):
    sense, steps = SENSE[core], STEPS[core]
    near = [(0, steps), (sign, steps)]
    near += [(2 * sign * way * sense, steps[part]) for way, part in TWO_AWAY] + [(-sign, steps)]
    return [(z + d + sign * sense * NEAR * k) % (FAR * NEAR) for d, ks in near for k in ks]


def devices(n, sign):
    cores = [n % 2, 1 - n % 2]
    return [z * 2 + (c ^ p) for c in cores for z in places(n // 2, c, sign) for p in range(2)]


def arrival(n):
    return devices(n, -1)


def departure(n):
    return devices(n, 1)


def summed(kept, sent):
    kept = kept + other_core(sent).astype(f32)
    sent = kept.astype(bf16)
    with_it, against = two_away_terms(sent[2])
    up, down = along_z(sent[1], (1, 1)), along_z(sent[3], (-1, -1))
    terms = [kept[0, k] + up[k].astype(f32) + down[k].astype(f32) for k in range(4)]
    terms[1] += against[0].astype(f32)
    terms[2] += with_it[0].astype(f32) + against[1].astype(f32)
    terms[3] += with_it[1].astype(f32)
    total = passed_on(terms[0].astype(bf16), (1,)).astype(f32)
    for k in (3, 2, 1):
        total = passed_on((total + terms[k]).astype(bf16)).astype(f32)
    total += of_core(terms[0], 0.0)
    return total + other_core(total)[::-1]


def two_away_terms(x):
    return [along_z(x[2 * i : 2 * i + 2], (-2 * way, 2 * way)) for i, (way, _) in enumerate(TWO_AWAY)]


def whole_attention(queries, keys, values, live_lengths, score_scale):
    scores = jnp.einsum("egc,etc->egt", queries, keys, preferred_element_type=f32) * score_scale
    live_mask = (
        jnp.arange(keys.shape[1], dtype=jnp.int32)[None, None, :] < live_lengths[:, None, None]
    )
    scores = jnp.where(live_mask, scores, -1e30)
    running_max = jnp.max(scores, axis=-1, keepdims=True)
    weights = jnp.where(live_mask, jnp.exp(scores - running_max), 0.0)
    probs = (weights / jnp.sum(weights, axis=-1, keepdims=True)).astype(bf16)
    return jnp.einsum("egt,etc->egc", probs, values, preferred_element_type=f32).astype(bf16)


def nt_dot(a, b):
    return lax.dot_general(a, b, (((1,), (1,)), ((), ())), preferred_element_type=f32)


def rows_of(g):
    return pl.ds(pl.multiple_of(g * SHARE, SHARE), SHARE)


def up_kernel(
    order, active, mine, theirs, residual, out_t, gain, gate, up,
    stream, kept, sent, heads, squares, gates, ups, both, arrived,
):
    groups = active.shape[0]
    half = DEVICES // 2
    cols = gate.shape[1] // CHUNKS
    copies = []
    for i in range(CHUNKS):
        at = pl.ds(i * cols, cols)
        copies.append([
            pltpu.make_async_copy(gate.at[:, at], gates.at[:, at], arrived.at[0, i]),
            pltpu.make_async_copy(up.at[:, at], ups.at[:, at], arrived.at[1, i]),
        ])
        for copy in copies[-1]:
            copy.start()

    for x, buf in enumerate((mine, theirs)):

        @pl.loop(0, half, unroll=UNROLL)
        def _(i):
            device = order[0, x * half + i]
            heads[device // groups, lax.rem(device, groups)] = buf[i].astype(f32)

    width = heads.shape[-1]
    total = residual[...].astype(f32)
    for h in range(heads.shape[0]):
        lhs = heads[h].reshape(ROWS, width).astype(bf16)
        total += nt_dot(lhs, out_t[:, h * width : (h + 1) * width])
    stream[...] = total
    lane = lax.broadcasted_iota(jnp.int32, (ROWS, LANES), 1).astype(f32)
    ones = 1.0 + lane / LANES
    squares[...] = jnp.sum(total * total, axis=1, keepdims=True) * ones
    scaled = total * gain[...]
    high = scaled.astype(bf16)
    low = (scaled - high.astype(f32)).astype(bf16)
    lhs = jnp.concatenate([high, low], axis=1)

    for i in range(CHUNKS):
        for t, w in enumerate((gates, ups)):
            copies[i][t].wait()
            rhs = w[:, i * cols : (i + 1) * cols]
            out = jnp.dot(lhs, jnp.concatenate([rhs, rhs], axis=0), preferred_element_type=f32)
            for j in range(cols // BLK):
                both[i * (cols // BLK) + j, :, t * BLK : (t + 1) * BLK] = out[:, j * BLK : (j + 1) * BLK]

    for x, to in enumerate((kept, sent)):

        @pl.loop(0, half, unroll=UNROLL)
        def _(i):
            device = order[1, x * half + i]
            q, g = device // groups, lax.rem(device, groups)
            rows = rows_of(g)
            for j in range(SHARE):
                tile = both[active[g, q * SHARE + j], rows, :].astype(to.dtype)
                to[i, :, j * BLK : (j + 1) * BLK] = tile[:, :BLK]
                to[i, :, (SHARE + j) * BLK : (SHARE + j + 1) * BLK] = tile[:, BLK:]
            to[i, :, 2 * SHARE * BLK :] = squares[rows, :].astype(to.dtype)


def down_kernel(order, active, mine, theirs, stream_t, down_hbm, out_t, dense, down_t, arrived):
    groups = active.shape[0]
    half = DEVICES // 2
    cols = down_t.shape[1] // CHUNKS
    copies = []
    for i in range(CHUNKS):
        at = pl.ds(i * cols, cols)
        copies.append(pltpu.make_async_copy(down_hbm.at[:, at], down_t.at[:, at], arrived.at[i]))
        copies[-1].start()
    dense[...] = jnp.zeros_like(dense)
    for x, buf in enumerate((mine, theirs)):

        @pl.loop(0, half, unroll=UNROLL)
        def _(i):
            device = order[0, x * half + i]
            q, g = device // groups, lax.rem(device, groups)
            rows = rows_of(g)
            tile = buf[i].astype(f32)
            for j in range(SHARE):
                dense[active[g, q * SHARE + j], rows, :] = tile[:, j * BLK : (j + 1) * BLK]

    total = stream_t[...]
    per = 4
    for k in range(dense.shape[0] // per):
        if k * per * BLK % cols == 0:
            copies[k * per * BLK // cols].wait()
        rhs = jnp.concatenate([dense[k * per + j].astype(bf16) for j in range(per)], axis=1)
        total += nt_dot(down_t[:, k * per * BLK : (k + 1) * per * BLK], rhs)
    out_t[...] = total.astype(out_t.dtype)


SMEM = pl.BlockSpec(memory_space=pltpu.SMEM)
VMEM = pl.BlockSpec(memory_space=pltpu.VMEM)
HBM = pl.BlockSpec(memory_space=pltpu.HBM)


def body(
    queries,
    keys,
    values,
    lengths,
    active_blocks,
    residual,
    out_weight,
    norm_gain,
    gate_weight,
    up_weight,
    down_weight,
):
    entries = keys.shape[0]
    me = lax.axis_index(AXES)
    tables = np.array([[arrival(n), departure(n)] for n in range(DEVICES)], np.int32)
    order = lax.dynamic_index_in_dim(jnp.asarray(tables), me, keepdims=False)
    live_lengths = lax.dynamic_slice_in_dim(lengths, (me * entries) % ROWS, entries)
    attended = whole_attention(queries, keys, values, live_lengths, queries.shape[2] ** (-0.5))
    attended = attended.reshape(entries, -1)
    width = residual.shape[1]
    ready = (order, residual, norm_gain.astype(f32).reshape(1, width))
    mine, theirs, ready = gathered(jnp.stack([attended, other_core(attended)]), ready)
    order, residual, gain = ready

    width = residual.shape[1]
    half = DEVICES // 2
    features = mine.shape[-1]
    share_cols = 2 * SHARE * BLK + LANES
    flat = (half, SHARE, features)
    stream, kept, sent = pl.pallas_call(
        up_kernel,
        in_specs=[SMEM, SMEM, VMEM, VMEM, VMEM, VMEM, VMEM, HBM, HBM],
        out_specs=[VMEM, VMEM, VMEM],
        out_shape=[
            jax.ShapeDtypeStruct((ROWS, width), f32),
            jax.ShapeDtypeStruct((half, SHARE, share_cols), f32),
            jax.ShapeDtypeStruct((half, SHARE, share_cols), bf16),
        ],
        scratch_shapes=[
            pltpu.VMEM((out_weight.shape[0] // features, ROWS // SHARE, SHARE, features), f32),
            pltpu.VMEM((ROWS, LANES), f32),
            pltpu.VMEM(gate_weight.shape, bf16),
            pltpu.VMEM(up_weight.shape, bf16),
            pltpu.VMEM((gate_weight.shape[1] // BLK, ROWS, 2 * BLK), f32),
            pltpu.SemaphoreType.DMA((2, CHUNKS)),
        ],
        compiler_params=pltpu.CompilerParams(vmem_limit_bytes=VMEM_LIMIT),
        name="up_kernel",
    )(
        order,
        active_blocks,
        mine.reshape(flat),
        theirs.reshape(flat),
        residual,
        out_weight.T,
        gain,
        gate_weight,
        up_weight,
    )

    terms = (NEAR, FAR // 2, 2, SHARE, share_cols)
    share = summed(kept.reshape(terms), sent.reshape(terms))
    cols = SHARE * BLK
    weights = 1.0 + jnp.arange(LANES, dtype=f32) / LANES
    square_sums = jnp.sum(share[..., 2 * cols :], axis=-1, keepdims=True) / jnp.sum(weights)
    inverse = 1.0 / (square_sums / D + 1e-05)
    activated = jnp.maximum(share[..., :cols], 0.0) * share[..., cols : 2 * cols] * inverse
    mine, theirs, _ = gathered(activated.astype(bf16))

    return pl.pallas_call(
        down_kernel,
        in_specs=[SMEM, SMEM, VMEM, VMEM, VMEM, HBM],
        out_specs=VMEM,
        out_shape=jax.ShapeDtypeStruct((width, ROWS), bf16),
        scratch_shapes=[
            pltpu.VMEM((down_weight.shape[0] // BLK, ROWS, BLK), f32),
            pltpu.VMEM((width, down_weight.shape[0]), bf16),
            pltpu.SemaphoreType.DMA((CHUNKS,)),
        ],
        compiler_params=pltpu.CompilerParams(vmem_limit_bytes=VMEM_LIMIT),
        name="down_kernel",
    )(order, active_blocks, mine.reshape(flat), theirs.reshape(flat), stream.T, down_weight.T).T


def solution(mesh):
    split = Mesh(mesh.devices.reshape(mesh.shape["groups"], FAR, NEAR, 2), ALL)
    return jax.shard_map(
        body,
        mesh=split,
        in_specs=(
            P(ALL, None, None),
            P(ALL, None, None),
            P(ALL, None, None),
            P("groups"),
            P("groups", None),
            P("groups", AXES),
            P(None, AXES),
            P(AXES),
            P(AXES, None),
            P(AXES, None),
            P(None, AXES),
        ),
        out_specs=P("groups", AXES),
        check_vma=False,
    )
```

```python
import jax
import jax.numpy as jnp
import numpy as np
from jax import lax
from jax.experimental import pallas as pl
from jax.experimental.pallas import tpu as pltpu
from jax.sharding import Mesh
from jax.sharding import PartitionSpec as P

D = 4096
BLK = 128
ROWS = 128
FAR, NEAR = 8, 4
DEVICES = FAR * NEAR * 2
SHARE = 8
LANES = 128
CHUNKS = 7
VMEM_LIMIT = 55 * 1024 * 1024
UNROLL = 4
AXES = ("far", "near", "core")
ALL = ("groups",) + AXES
f32, bf16 = jnp.float32, jnp.bfloat16

SENSE = (-1, 1)
STEPS = ((0, 1, 2, 3), (4, 1, 2, 3))
TWO_AWAY = ((1, slice(2, 4)), (-1, slice(1, 3)))


def along_z(x, steps, cores=(0, 1)):
    chips = FAR * NEAR
    pairs = [(2 * z + c, (z + steps[c]) % chips * 2 + c) for z in range(chips) for c in cores]
    return lax.ppermute(x, AXES, pairs)


def passed_on(x, cores=(0, 1)):
    return along_z(x, (-NEAR, NEAR), cores)


def two_away(x):
    return [along_z(x[part], (-2 * way, 2 * way)) for way, part in TWO_AWAY]


def other_core(x):
    return lax.ppermute(x, "core", [(0, 1), (1, 0)])


def of_core(first, second):
    return jnp.where(lax.axis_index("core") == 0, first, second)


def gathered(pair, ready=None):
    held = [pair, passed_on(pair)]
    if ready is not None:
        held[1], ready = lax.optimization_barrier((held[1], ready))
    for k in range(2):
        held.append(passed_on(held[-1]))
    held[0] = of_core(pair, passed_on(held[-1], (1,)))
    far = jnp.stack(held)
    near = [far, along_z(far, (1, 1)), jnp.concatenate(two_away(far)), along_z(far, (-1, -1))]
    near = jnp.stack(near)
    return near, other_core(near), ready


def places(z, core, sign):
    sense, steps = SENSE[core], STEPS[core]
    near = [(0, steps), (sign, steps)]
    near += [(2 * sign * way * sense, steps[part]) for way, part in TWO_AWAY] + [(-sign, steps)]
    return [(z + d + sign * sense * NEAR * k) % (FAR * NEAR) for d, ks in near for k in ks]


def devices(n, sign):
    cores = [n % 2, 1 - n % 2]
    return [z * 2 + (c ^ p) for c in cores for z in places(n // 2, c, sign) for p in range(2)]


def arrival(n):
    return devices(n, -1)


def departure(n):
    return devices(n, 1)


def summed(kept, sent):
    kept = kept + other_core(sent).astype(f32)
    sent = kept.astype(bf16)
    with_it, against = two_away_terms(sent[2])
    up, down = along_z(sent[1], (1, 1)), along_z(sent[3], (-1, -1))
    terms = [kept[0, k] + up[k].astype(f32) + down[k].astype(f32) for k in range(4)]
    terms[1] += against[0].astype(f32)
    terms[2] += with_it[0].astype(f32) + against[1].astype(f32)
    terms[3] += with_it[1].astype(f32)
    total = passed_on(terms[0].astype(bf16), (1,)).astype(f32)
    for k in (3, 2, 1):
        total = passed_on((total + terms[k]).astype(bf16)).astype(f32)
    total += of_core(terms[0], 0.0)
    return total + other_core(total)[::-1]


def two_away_terms(x):
    return [along_z(x[2 * i : 2 * i + 2], (-2 * way, 2 * way)) for i, (way, _) in enumerate(TWO_AWAY)]


def whole_attention(queries, keys, values, live_lengths, score_scale):
    scores = jnp.einsum("egc,etc->egt", queries, keys, preferred_element_type=f32) * score_scale
    live_mask = (
        jnp.arange(keys.shape[1], dtype=jnp.int32)[None, None, :] < live_lengths[:, None, None]
    )
    scores = jnp.where(live_mask, scores, -1e30)
    running_max = jnp.max(scores, axis=-1, keepdims=True)
    weights = jnp.where(live_mask, jnp.exp(scores - running_max), 0.0)
    probs = (weights / jnp.sum(weights, axis=-1, keepdims=True)).astype(bf16)
    return jnp.einsum("egt,etc->egc", probs, values, preferred_element_type=f32).astype(bf16)


def nt_dot(a, b):
    return lax.dot_general(a, b, (((1,), (1,)), ((), ())), preferred_element_type=f32)


def rows_of(g):
    return pl.ds(pl.multiple_of(g * SHARE, SHARE), SHARE)


def up_kernel(
    order, active, mine, theirs, residual, out_t, gain, gate, up,
    stream, kept, sent, heads, squares, gates, ups, both, arrived,
):
    groups = active.shape[0]
    half = DEVICES // 2
    cols = gate.shape[1] // CHUNKS
    copies = []
    for i in range(CHUNKS):
        at = pl.ds(i * cols, cols)
        copies.append([
            pltpu.make_async_copy(gate.at[:, at], gates.at[:, at], arrived.at[0, i]),
            pltpu.make_async_copy(up.at[:, at], ups.at[:, at], arrived.at[1, i]),
        ])
        for copy in copies[-1]:
            copy.start()

    for x, buf in enumerate((mine, theirs)):

        @pl.loop(0, half, unroll=UNROLL)
        def _(i):
            device = order[0, x * half + i]
            heads[device // groups, lax.rem(device, groups)] = buf[i].astype(f32)

    width = heads.shape[-1]
    total = residual[...].astype(f32)
    for h in range(heads.shape[0]):
        lhs = heads[h].reshape(ROWS, width).astype(bf16)
        total += nt_dot(lhs, out_t[:, h * width : (h + 1) * width])
    stream[...] = total
    lane = lax.broadcasted_iota(jnp.int32, (ROWS, LANES), 1).astype(f32)
    ones = 1.0 + lane / LANES
    squares[...] = jnp.sum(total * total, axis=1, keepdims=True) * ones
    scaled = total * gain[...]
    high = scaled.astype(bf16)
    low = (scaled - high.astype(f32)).astype(bf16)
    lhs = jnp.concatenate([high, low], axis=1)

    for i in range(CHUNKS):
        for t, w in enumerate((gates, ups)):
            copies[i][t].wait()
            rhs = w[:, i * cols : (i + 1) * cols]
            out = jnp.dot(lhs, jnp.concatenate([rhs, rhs], axis=0), preferred_element_type=f32)
            for j in range(cols // BLK):
                both[i * (cols // BLK) + j, :, t * BLK : (t + 1) * BLK] = out[:, j * BLK : (j + 1) * BLK]

    for x, to in enumerate((kept, sent)):

        @pl.loop(0, half, unroll=UNROLL)
        def _(i):
            device = order[1, x * half + i]
            q, g = device // groups, lax.rem(device, groups)
            rows = rows_of(g)
            for j in range(SHARE):
                tile = both[active[g, q * SHARE + j], rows, :].astype(to.dtype)
                to[i, :, j * BLK : (j + 1) * BLK] = tile[:, :BLK]
                to[i, :, (SHARE + j) * BLK : (SHARE + j + 1) * BLK] = tile[:, BLK:]
            to[i, :, 2 * SHARE * BLK :] = squares[rows, :].astype(to.dtype)


def down_kernel(order, active, mine, theirs, stream_t, down_hbm, out_t, dense, down_t, arrived):
    groups = active.shape[0]
    half = DEVICES // 2
    cols = down_t.shape[1] // CHUNKS
    copies = []
    for i in range(CHUNKS):
        at = pl.ds(i * cols, cols)
        copies.append(pltpu.make_async_copy(down_hbm.at[:, at], down_t.at[:, at], arrived.at[i]))
        copies[-1].start()
    dense[...] = jnp.zeros_like(dense)
    for x, buf in enumerate((mine, theirs)):

        @pl.loop(0, half, unroll=UNROLL)
        def _(i):
            device = order[0, x * half + i]
            q, g = device // groups, lax.rem(device, groups)
            rows = rows_of(g)
            tile = buf[i].astype(f32)
            for j in range(SHARE):
                dense[active[g, q * SHARE + j], rows, :] = tile[:, j * BLK : (j + 1) * BLK]

    total = stream_t[...]
    per = 8
    for k in range(dense.shape[0] // per):
        if k * per * BLK % cols == 0:
            copies[k * per * BLK // cols].wait()
        rhs = jnp.concatenate([dense[k * per + j].astype(bf16) for j in range(per)], axis=1)
        total += nt_dot(down_t[:, k * per * BLK : (k + 1) * per * BLK], rhs)
    out_t[...] = total.astype(out_t.dtype)


SMEM = pl.BlockSpec(memory_space=pltpu.SMEM)
VMEM = pl.BlockSpec(memory_space=pltpu.VMEM)
HBM = pl.BlockSpec(memory_space=pltpu.HBM)


def body(
    queries,
    keys,
    values,
    lengths,
    active_blocks,
    residual,
    out_weight,
    norm_gain,
    gate_weight,
    up_weight,
    down_weight,
):
    entries = keys.shape[0]
    me = lax.axis_index(AXES)
    tables = np.array([[arrival(n), departure(n)] for n in range(DEVICES)], np.int32)
    order = lax.dynamic_index_in_dim(jnp.asarray(tables), me, keepdims=False)
    live_lengths = lax.dynamic_slice_in_dim(lengths, (me * entries) % ROWS, entries)
    attended = whole_attention(queries, keys, values, live_lengths, queries.shape[2] ** (-0.5))
    attended = attended.reshape(entries, -1)
    width = residual.shape[1]
    ready = (order, residual, norm_gain.astype(f32).reshape(1, width))
    mine, theirs, ready = gathered(jnp.stack([attended, other_core(attended)]), ready)
    order, residual, gain = ready

    width = residual.shape[1]
    half = DEVICES // 2
    features = mine.shape[-1]
    share_cols = 2 * SHARE * BLK + LANES
    flat = (half, SHARE, features)
    stream, kept, sent = pl.pallas_call(
        up_kernel,
        in_specs=[SMEM, SMEM, VMEM, VMEM, VMEM, VMEM, VMEM, HBM, HBM],
        out_specs=[VMEM, VMEM, VMEM],
        out_shape=[
            jax.ShapeDtypeStruct((ROWS, width), f32),
            jax.ShapeDtypeStruct((half, SHARE, share_cols), f32),
            jax.ShapeDtypeStruct((half, SHARE, share_cols), bf16),
        ],
        scratch_shapes=[
            pltpu.VMEM((out_weight.shape[0] // features, ROWS // SHARE, SHARE, features), f32),
            pltpu.VMEM((ROWS, LANES), f32),
            pltpu.VMEM(gate_weight.shape, bf16),
            pltpu.VMEM(up_weight.shape, bf16),
            pltpu.VMEM((gate_weight.shape[1] // BLK, ROWS, 2 * BLK), f32),
            pltpu.SemaphoreType.DMA((2, CHUNKS)),
        ],
        compiler_params=pltpu.CompilerParams(vmem_limit_bytes=VMEM_LIMIT),
        name="up_kernel",
    )(
        order,
        active_blocks,
        mine.reshape(flat),
        theirs.reshape(flat),
        residual,
        out_weight.T,
        gain,
        gate_weight,
        up_weight,
    )

    terms = (NEAR, FAR // 2, 2, SHARE, share_cols)
    share = summed(kept.reshape(terms), sent.reshape(terms))
    cols = SHARE * BLK
    weights = 1.0 + jnp.arange(LANES, dtype=f32) / LANES
    square_sums = jnp.sum(share[..., 2 * cols :], axis=-1, keepdims=True) / jnp.sum(weights)
    inverse = 1.0 / (square_sums / D + 1e-05)
    activated = jnp.maximum(share[..., :cols], 0.0) * share[..., cols : 2 * cols] * inverse
    mine, theirs, _ = gathered(activated.astype(bf16))

    return pl.pallas_call(
        down_kernel,
        in_specs=[SMEM, SMEM, VMEM, VMEM, VMEM, HBM],
        out_specs=VMEM,
        out_shape=jax.ShapeDtypeStruct((width, ROWS), bf16),
        scratch_shapes=[
            pltpu.VMEM((down_weight.shape[0] // BLK, ROWS, BLK), f32),
            pltpu.VMEM((width, down_weight.shape[0]), bf16),
            pltpu.SemaphoreType.DMA((CHUNKS,)),
        ],
        compiler_params=pltpu.CompilerParams(vmem_limit_bytes=VMEM_LIMIT),
        name="down_kernel",
    )(order, active_blocks, mine.reshape(flat), theirs.reshape(flat), stream.T, down_weight.T).T


def solution(mesh):
    split = Mesh(mesh.devices.reshape(mesh.shape["groups"], FAR, NEAR, 2), ALL)
    return jax.shard_map(
        body,
        mesh=split,
        in_specs=(
            P(ALL, None, None),
            P(ALL, None, None),
            P(ALL, None, None),
            P("groups"),
            P("groups", None),
            P("groups", AXES),
            P(None, AXES),
            P(AXES),
            P(AXES, None),
            P(AXES, None),
            P(None, AXES),
        ),
        out_specs=P("groups", AXES),
        check_vma=False,
    )
```
